32 devices in a mesh: dp: 4 (over y, z), tp: 8 (over x, core).
Axes of the slice: x: 4, y: 2, z: 2, core: 2. Of those that a mesh axis runs over, the one named last changes fastest.
The devices are a block of a 4x4x8 slice.
Arguments:
- hidden: bfloat16 [1024, 4096], P('dp'), parts along dimension 0
- w_q: bfloat16 [4096, 4096], P(None, 'tp')
- w_k: bfloat16 [4096, 4096], P(None, 'tp')
- w_v: bfloat16 [4096, 4096], P(None, 'tp')
- w_o: bfloat16 [4096, 4096], P('tp')
- q_norm_w: float32 [4096], P('tp')
- k_norm_w: float32 [4096], P('tp')
- post_norm_w: float32 [4096], replicated
- k_cache: bfloat16 [1024, 32, 32, 128], P('dp', None, 'tp'), parts along dimension 0
- v_cache: bfloat16 [1024, 32, 32, 128], P('dp', None, 'tp'), parts along dimension 0
- positions: int32 [1024], P('dp'), parts along dimension 0
Outputs:
- output 1: bfloat16 [1024, 4096], P('dp'), parts along dimension 0
- output 2: bfloat16 [1024, 32, 32, 128], P('dp', None, 'tp'), parts along dimension 0
- output 3: bfloat16 [1024, 32, 32, 128], P('dp', None, 'tp'), parts along dimension 0
There are 4 independent parts. The reference program is written for one: setup_inputs(seed, part) draws one part's arguments, and reference() takes and returns one part's arrays. A program takes and returns all parts, laid end to end along the dimension named above; an argument that names none is the same for every part.
All inputs are finite; a program needn't handle non-finite values.
Results may differ from the reference program's by a relative error of at most 0.0120168.
Values are sent between devices in bfloat16 or wider.
A program may use at most 768 MiB of HBM per device.

```python
import jax
import jax.numpy as jnp
from jax import lax

BATCH = 256
CACHE_LEN = 32
HEADS = 32
HEAD_DIM = 128
WIDTH = HEADS * HEAD_DIM
NORM_EPS = 1e-6
ROPE_BASE = 500000.0


def setup_inputs(seed: int = 0, part: int = 0) -> dict:
    base_key = jax.random.key(seed)
    shared_keys = jax.random.split(base_key, 9)
    part_keys = jax.random.split(jax.random.fold_in(base_key, part), 6)
    fan_scale = WIDTH ** -0.5
    head_frac = jnp.arange(HEADS, dtype=jnp.float32) / max(HEADS - 1, 1)
    q_heads = jnp.exp(1.2 * (2.0 * head_frac - 1.0) + 0.2 * jax.random.normal(shared_keys[0], (HEADS,)))
    k_heads = jnp.exp(1.2 * (1.0 - 2.0 * head_frac) + 0.2 * jax.random.normal(shared_keys[1], (HEADS,)))
    q_cols = jnp.repeat(q_heads, HEAD_DIM)
    k_cols = jnp.repeat(k_heads, HEAD_DIM)
    w_q = (jax.random.normal(shared_keys[2], (WIDTH, WIDTH)) * fan_scale * q_cols[None, :]).astype(jnp.bfloat16)
    w_k = (jax.random.normal(shared_keys[3], (WIDTH, WIDTH)) * fan_scale * k_cols[None, :]).astype(jnp.bfloat16)
    w_v = (jax.random.normal(shared_keys[4], (WIDTH, WIDTH)) * fan_scale).astype(jnp.bfloat16)
    w_o = (jax.random.normal(shared_keys[5], (WIDTH, WIDTH)) * fan_scale).astype(jnp.bfloat16)
    q_norm_w = jax.random.uniform(shared_keys[6], (WIDTH,), minval=0.5, maxval=1.5).astype(jnp.float32)
    k_norm_w = jax.random.uniform(shared_keys[7], (WIDTH,), minval=0.5, maxval=1.5).astype(jnp.float32)
    post_norm_w = jax.random.uniform(shared_keys[8], (WIDTH,), minval=0.5, maxval=1.5).astype(jnp.float32)
    hidden = jax.random.normal(part_keys[0], (BATCH, WIDTH)).astype(jnp.bfloat16)
    k_cache = jax.random.normal(part_keys[1], (BATCH, CACHE_LEN, HEADS, HEAD_DIM)).astype(jnp.bfloat16)
    v_cache = jax.random.normal(part_keys[2], (BATCH, CACHE_LEN, HEADS, HEAD_DIM)).astype(jnp.bfloat16)
    slot_draw = jax.random.randint(part_keys[3], (BATCH,), 0, CACHE_LEN, dtype=jnp.int32)
    shift_bits = jax.random.randint(part_keys[4], (BATCH,), 0, 10, dtype=jnp.int32)
    longest = jax.random.randint(part_keys[5], (), 0, BATCH, dtype=jnp.int32)
    positions = jnp.where(jnp.arange(BATCH, dtype=jnp.int32) == longest, CACHE_LEN - 1, jnp.right_shift(slot_draw, shift_bits)).astype(jnp.int32)
    return dict(hidden=hidden, w_q=w_q, w_k=w_k, w_v=w_v, w_o=w_o, q_norm_w=q_norm_w, k_norm_w=k_norm_w, post_norm_w=post_norm_w, k_cache=k_cache, v_cache=v_cache, positions=positions)


def width_norm(vals, gain):
    wide = vals.astype(jnp.float32)
    inv_rms = lax.rsqrt(jnp.mean(wide * wide, axis=-1, keepdims=True) + NORM_EPS)
    return wide * inv_rms * gain


def apply_rope(heads_val, positions):
    half = HEAD_DIM // 2
    inv_freq = ROPE_BASE ** (-2.0 * jnp.arange(half, dtype=jnp.float32) / HEAD_DIM)
    angles = positions.astype(jnp.float32)[:, None, None] * inv_freq[None, None, :]
    cos_tab = jnp.cos(angles)
    sin_tab = jnp.sin(angles)
    wide = heads_val.astype(jnp.float32)
    first = wide[..., :half]
    second = wide[..., half:]
    return jnp.concatenate([first * cos_tab - second * sin_tab, second * cos_tab + first * sin_tab], axis=-1).astype(jnp.bfloat16)


def attend_row(row_args):
    q_row, k_row, v_row, row_pos = row_args
    slot_ids = jnp.arange(CACHE_LEN)
    scores = jnp.einsum('hd,shd->hs', q_row.astype(jnp.float32), k_row.astype(jnp.float32)) * HEAD_DIM ** -0.5
    scores = jnp.where(slot_ids[None, :] <= row_pos, scores, -1e30)
    probs = jax.nn.softmax(scores, axis=-1).astype(jnp.bfloat16)
    return jnp.einsum('hs,shd->hd', probs.astype(jnp.float32), v_row.astype(jnp.float32)).astype(jnp.bfloat16)


def reference(hidden, w_q, w_k, w_v, w_o, q_norm_w, k_norm_w, post_norm_w, k_cache, v_cache, positions):
    n_rows = hidden.shape[0]
    q_full = jnp.dot(hidden, w_q, preferred_element_type=jnp.float32).astype(jnp.bfloat16)
    k_full = jnp.dot(hidden, w_k, preferred_element_type=jnp.float32).astype(jnp.bfloat16)
    v_full = jnp.dot(hidden, w_v, preferred_element_type=jnp.float32).astype(jnp.bfloat16)
    q_normed = width_norm(q_full, q_norm_w).astype(jnp.bfloat16).reshape(n_rows, HEADS, HEAD_DIM)
    k_normed = width_norm(k_full, k_norm_w).astype(jnp.bfloat16).reshape(n_rows, HEADS, HEAD_DIM)
    q_rot = apply_rope(q_normed, positions)
    k_rot = apply_rope(k_normed, positions)
    v_heads = v_full.reshape(n_rows, HEADS, HEAD_DIM)
    at_slot = (jnp.arange(CACHE_LEN)[None, :] == positions[:, None])[:, :, None, None]
    k_new = jnp.where(at_slot, k_rot[:, None], k_cache)
    v_new = jnp.where(at_slot, v_heads[:, None], v_cache)
    attn = lax.map(attend_row, (q_rot, k_new, v_new, positions))
    a_out = jnp.dot(attn.reshape(n_rows, WIDTH), w_o, preferred_element_type=jnp.float32)
    hidden_out = (hidden.astype(jnp.float32) + width_norm(a_out, post_norm_w)).astype(jnp.bfloat16)
    return hidden_out, k_new, v_new
```

```python
import functools

import jax
import jax.numpy as jnp
from jax import lax
from jax.experimental import pallas as pl
from jax.experimental.pallas import tpu as pltpu
from jax.sharding import PartitionSpec as P

NORM_EPS = 1e-6
ROPE_BASE = 500000.0
MESH = pl.DeviceIdType.MESH
LANES = 128
F32 = jnp.float32
BF16 = jnp.bfloat16
K_CHUNKS = 4
GROUP = 16


def column(row_vals, count):
    blocks = []
    for i in range(count):
        block = jnp.broadcast_to(row_vals[i:i + 1, :], (LANES, LANES))
        blocks.append(block.T)
    return jnp.concatenate(blocks, axis=0) if count > 1 else blocks[0]


def project_kernel(n_tp, hidden, w_q, w_k, w_v, q_gain, k_gain, pos, freq, sign, q_out, k_out, v_out,
                   hbuf, wbuf, acc, cos_tab, sin_tab, e_send, e_recv, h_sems, w_sems, send_sems, recv_sems):
    me = lax.axis_index('tp')
    n_rows, width = hidden.shape
    cols = w_q.shape[1]
    heads = cols // LANES
    depth = width // K_CHUNKS

    def h_copy(c):
        part = pl.ds(c * depth, depth)
        return pltpu.make_async_copy(hidden.at[:, part], hbuf.at[c], h_sems.at[c])

    def w_copy(w, i, c):
        part = pl.ds(c * depth, depth)
        return pltpu.make_async_copy(w.at[part, :], wbuf.at[i * K_CHUNKS + c], w_sems.at[i * K_CHUNKS + c])

    for i, w in enumerate((w_q, w_k, w_v)):
        for c in range(K_CHUNKS):
            if i == 0:
                h_copy(c).start()
            w_copy(w, i, c).start()
    barrier = pltpu.get_barrier_semaphore()
    for d in range(1, n_tp):
        pl.semaphore_signal(barrier, inc=1, device_id={'tp': lax.rem(me + d, n_tp)}, device_id_type=MESH)

    angle = column(pos[...].astype(F32), n_rows // LANES) * freq[...]
    cos_tab[...] = jnp.cos(angle)
    sin_tab[...] = jnp.sin(angle) * sign[...]

    def matmul(i, w):
        def chunk(c, carry):
            @pl.when(i * K_CHUNKS + c < K_CHUNKS)
            def _():
                h_copy(c).wait()
            w_copy(w, i, c).wait()
            part = jnp.dot(hbuf[c], wbuf[i * K_CHUNKS + c], preferred_element_type=F32)
            @pl.when(c == 0)
            def _():
                acc[i] = part
            @pl.when(c > 0)
            def _():
                acc[i] = acc[i] + part
            return carry
        lax.fori_loop(0, K_CHUNKS, chunk, 0)

    matmul(0, w_q)
    matmul(1, w_k)
    lane = lax.broadcasted_iota(jnp.int32, (n_rows, LANES), 1)
    sums = []
    for i in range(2):
        wide = acc[i].astype(BF16).astype(F32)
        sums.append(jnp.sum(wide * wide, axis=1, keepdims=True))
    both = jnp.where(lane < 4, sums[0], sums[1])
    e_send[...] = both.T[0:8, :]
    pl.semaphore_wait(barrier, n_tp - 1)
    copies = []
    for d in range(1, n_tp):
        copies.append(pltpu.make_async_remote_copy(
            src_ref=e_send, dst_ref=e_recv.at[d - 1], send_sem=send_sems.at[d - 1], recv_sem=recv_sems.at[d - 1],
            device_id={'tp': lax.rem(me + d, n_tp)}, device_id_type=MESH))
        copies[-1].start()
    matmul(2, w_v)
    for h in range(heads):
        v_out[h] = acc[2, :, h * LANES:(h + 1) * LANES].astype(BF16)
    total = e_send[...]
    for d in range(1, n_tp):
        copies[d - 1].wait_recv()
        total = total + e_recv[d - 1]
    inv = lax.rsqrt(total / width + NORM_EPS)
    inv_cols = jnp.concatenate([inv] * (LANES // 8), axis=0).T
    cos_val = cos_tab[...]
    sin_val = sin_tab[...]
    for i, (gain, out) in enumerate(((q_gain, q_out), (k_gain, k_out))):
        inv_col = inv_cols[:, 4 * i:4 * i + 1]
        for h in range(heads):
            part = slice(h * LANES, (h + 1) * LANES)
            wide = acc[i, :, part].astype(BF16).astype(F32)
            normed = (wide * inv_col * gain[:, part]).astype(BF16).astype(F32)
            out[h] = (normed * cos_val + pltpu.roll(normed, LANES // 2, 1) * sin_val).astype(BF16)
    for copy in copies:
        copy.wait_send()


def attend_kernel(slots, heads, pos_smem, pos, q, k, v, k_cache, v_cache, k_new, v_new, o,
                  kbuf, vbuf, k_rows, v_rows, pos_col, in_sems, out_sems):
    n_rows = q.shape[1]
    span = slots * heads
    n_groups = n_rows // GROUP
    block = GROUP * span

    def in_copy(i, g):
        src, dst = ((k_cache, kbuf), (v_cache, vbuf))[i]
        part = pl.ds(g * block, block)
        return pltpu.make_async_copy(src.at[part, :], dst.at[part, :], in_sems.at[i, g])

    def out_copy(i, g):
        src, dst = ((kbuf, k_new), (vbuf, v_new))[i]
        part = pl.ds(g * block, block)
        return pltpu.make_async_copy(src.at[part, :], dst.at[part, :], out_sems.at[i, g])

    for g in range(n_groups):
        in_copy(0, g).start()
        in_copy(1, g).start()
    pos_col[...] = column(pos[...].astype(F32), n_rows // LANES)
    for src, dst in ((k, k_rows), (v, v_rows)):
        for r in range(8):
            dst[pl.ds(r, n_rows, stride=8), :] = src[r % heads].astype(F32)

    m_rows = heads * GROUP
    row_b = lax.broadcasted_iota(jnp.int32, (m_rows, LANES), 0) % GROUP
    row_h = lax.broadcasted_iota(jnp.int32, (m_rows, LANES), 0) // GROUP
    lane = lax.broadcasted_iota(jnp.int32, (m_rows, LANES), 1)
    own_head = (lane % heads) == row_h
    lane_slot = (lane // heads).astype(F32)
    tile_slot = lax.broadcasted_iota(jnp.int32, (16, LANES), 0) // heads
    per_tile = 16 // heads
    scale = LANES ** -0.5

    def group(g, carry):
        in_copy(0, g).wait()
        in_copy(1, g).wait()
        for b in range(GROUP):
            row = g * GROUP + b
            p = pos_smem[row]
            at = pl.multiple_of(row * span + (p // per_tile) * 16, 16)
            hit = tile_slot == p % per_tile
            for buf, rows in ((kbuf, k_rows), (vbuf, v_rows)):
                new = rows[pl.ds(pl.multiple_of(row * 8, 8), 8), :]
                new = jnp.concatenate([new, new], axis=0)
                old = buf[pl.ds(at, 16), :].astype(F32)
                buf[pl.ds(at, 16), :] = jnp.where(hit, new, old).astype(BF16)
        here = pl.ds(pl.multiple_of(g * block, block), block)
        rows_here = pl.ds(pl.multiple_of(g * GROUP, GROUP), GROUP)
        lhs = q[:, rows_here, :].reshape(m_rows, LANES)
        scores = lax.dot_general(lhs, kbuf[here, :], (((1,), (1,)), ((), ())), preferred_element_type=F32)
        mine = scores[:, 0:span]
        for b in range(1, GROUP):
            mine = jnp.where(row_b == b, scores[:, b * span:(b + 1) * span], mine)
        limit = pos_col[rows_here, :]
        limit = jnp.concatenate([limit] * heads, axis=0)
        mine = jnp.where(own_head & (lane_slot <= limit), mine * scale, -1e30)
        top = jnp.max(mine, axis=1, keepdims=True)
        e = jnp.exp(mine - top)
        probs = e / jnp.sum(e, axis=1, keepdims=True)
        wide = jnp.concatenate([jnp.where(row_b == b, probs, 0.0).astype(BF16) for b in range(GROUP)], axis=1)
        mixed = jnp.dot(wide, vbuf[here, :], preferred_element_type=F32).astype(BF16)
        for h in range(heads):
            o[rows_here, h * LANES:(h + 1) * LANES] = mixed[h * GROUP:(h + 1) * GROUP, :]
        out_copy(0, g).start()
        out_copy(1, g).start()
        return carry

    lax.fori_loop(0, n_groups, group, 0)
    for g in range(n_groups):
        out_copy(0, g).wait()
        out_copy(1, g).wait()


def combine_kernel(n_tp, n_chunks, o, w_o, hidden, gain, out,
                   wbuf, obuf, sib_send, sib_recv, own, ring_send, far_recv, near_send, near_recv,
                   w_sems, h_sem, hbuf, sib_s, sib_r, far_s, far_r, imm_s, imm_r, dep_s, dep_r, ag_s, ag_r):
    me = lax.axis_index('tp')
    chips = n_tp // 2
    x, c = me // 2, me % 2
    n_rows, width = hidden.shape
    half = width // 2
    blk = n_rows // n_chunks // n_tp
    side_rows = blk * chips
    chunk_rows = n_rows // n_chunks
    tile = 512
    n_tiles = width // tile
    right_x, left_x, far_x = lax.rem(x + 1, chips), lax.rem(x + chips - 1, chips), lax.rem(x + 2, chips)
    sib = {'tp': 2 * x + 1 - c}
    right = {'tp': 2 * right_x + c}
    left = {'tp': 2 * left_x + c}

    def w_copy(n):
        part = pl.ds(n * tile, tile)
        return pltpu.make_async_copy(w_o.at[:, part], wbuf.at[n], w_sems.at[n])

    for n in range(n_tiles):
        w_copy(n).start()
    barrier = pltpu.get_barrier_semaphore()
    for peer in (sib, right, left):
        pl.semaphore_signal(barrier, inc=1, device_id=peer, device_id_type=MESH)

    def remote(src, dst, s, r, peer):
        return pltpu.make_async_remote_copy(src_ref=src, dst_ref=dst, send_sem=s, recv_sem=r, device_id=peer, device_id_type=MESH)

    def block_of(which):
        return pl.ds(pl.multiple_of(which * blk, blk), blk)

    def out_rows(j, core, which):
        return pl.ds(pl.multiple_of(j * chunk_rows + core * side_rows + which * blk, blk), blk)

    def sib_copy(j, s):
        return remote(sib_send.at[j, s], sib_recv.at[j, s], sib_s.at[j, s], sib_r.at[j, s], sib)

    fwd = (right, left)

    def far_copy(j, s):
        return remote(ring_send.at[j, s], far_recv.at[j, s], far_s.at[j, s], far_r.at[j, s], fwd[s])

    def imm_copy(j, s):
        return remote(near_send.at[j, s, 1 - s], near_recv.at[j, s, 1 - s], imm_s.at[j, s], imm_r.at[j, s], fwd[s])

    def dep_copy(j, s):
        return remote(near_send.at[j, s, s], near_recv.at[j, s, s], dep_s.at[j, s], dep_r.at[j, s], fwd[s])

    fwd_x = (right_x, left_x)
    back_x = (left_x, right_x)

    def ag_copy(j, kind):
        if kind < 2:
            rows, part, peer = out_rows(j, c, x), slice(None), fwd[kind]
        elif kind < 4:
            s = kind - 2
            rows, part, peer = out_rows(j, c, back_x[s]), pl.ds(s * half, half), fwd[s]
        elif kind == 4:
            rows, part, peer = out_rows(j, c, x), slice(None), sib
        elif kind < 7:
            rows, part, peer = out_rows(j, c, back_x[kind - 5]), slice(None), sib
        else:
            rows, part, peer = out_rows(j, c, far_x), pl.ds((kind - 7) * half, half), sib
        ref = out.at[rows, part]
        return remote(ref, ref, ag_s.at[j, kind], ag_r.at[j, kind], peer)

    h_copies = []
    for j in range(n_chunks):
        rows = out_rows(j, c, x)
        h_copies.append(pltpu.make_async_copy(hidden.at[rows, :], hbuf.at[j], h_sem.at[j]))
        h_copies[-1].start()

    def project(j):
        mine = pl.ds(pl.multiple_of(j * chunk_rows + c * side_rows, side_rows), side_rows)
        theirs = pl.ds(pl.multiple_of(j * chunk_rows + (1 - c) * side_rows, side_rows), side_rows)
        obuf[0:side_rows, :] = o[theirs, :]
        obuf[side_rows:, :] = o[mine, :]
        for s in range(2):
            def tiles(n, carry):
                idx = s * (n_tiles // 2) + n
                if j == 0:
                    w_copy(idx).wait()
                part = jnp.dot(obuf[...], wbuf[idx], preferred_element_type=F32)
                at = pl.ds(pl.multiple_of(n * tile, tile), tile)
                sib_send[j, s, :, at] = part[0:side_rows].astype(BF16)
                own[j, s, :, at] = part[side_rows:]
                return carry
            lax.fori_loop(0, n_tiles // 2, tiles, 0)
            if j == 0 and s == 0:
                pl.semaphore_wait(barrier, 3)
            sib_copy(j, s).start()

    def chip_sum(j, s, which):
        rows = block_of(which)
        return own[j, s, rows, :] + sib_recv[j, s, rows, :].astype(F32)

    def scatter(j):
        for s in range(2):
            sib_copy(j, s).wait_recv()
            ring_send[j, s] = chip_sum(j, s, far_x).astype(BF16)
            far_copy(j, s).start()
        for s in range(2):
            near_send[j, s, 1 - s] = chip_sum(j, 1 - s, fwd_x[s]).astype(BF16)
            imm_copy(j, s).start()

    def relay(j):
        for s in range(2):
            far_copy(j, s).wait_recv()
            near_send[j, s, s] = (chip_sum(j, s, fwd_x[s]) + far_recv[j, s].astype(F32)).astype(BF16)
            dep_copy(j, s).start()

    def finish(j):
        parts = []
        h_copies[j].wait()
        for s in range(2):
            imm_copy(j, s).wait_recv()
            dep_copy(j, s).wait_recv()
        energy = 0.0
        for s in range(2):
            a = chip_sum(j, s, x) + near_recv[j, 0, s].astype(F32) + near_recv[j, 1, s].astype(F32)
            parts.append(a)
            energy = energy + jnp.sum(a * a, axis=1, keepdims=True)
        inv = lax.rsqrt(energy / width + NORM_EPS)
        rows = out_rows(j, c, x)
        for s in range(2):
            part = slice(s * half, (s + 1) * half)
            out[rows, part] = (hbuf[j, :, part].astype(F32) + parts[s] * inv * gain[:, part]).astype(BF16)

    def gather_first(j):
        for kind in (0, 1, 4):
            ag_copy(j, kind).start()

    def gather_relay(j):
        for s in range(2):
            ag_copy(j, s).wait_recv()
            ag_copy(j, 2 + s).start()
            ag_copy(j, 5 + s).start()

    def gather_last(j):
        for s in range(2):
            ag_copy(j, 2 + s).wait_recv()
            ag_copy(j, 7 + s).start()

    project(0)
    scatter(0)
    project(1)
    relay(0)
    scatter(1)
    finish(0)
    gather_first(0)
    relay(1)
    gather_relay(0)
    finish(1)
    gather_first(1)
    gather_last(0)
    gather_relay(1)
    gather_last(1)
    for j in range(n_chunks):
        for kind in range(4, 9):
            ag_copy(j, kind).wait_recv()
        for s in range(2):
            sib_copy(j, s).wait_send()
            far_copy(j, s).wait_send()
            imm_copy(j, s).wait_send()
            dep_copy(j, s).wait_send()
        for kind in range(9):
            ag_copy(j, kind).wait_send()


VMEM = pl.BlockSpec(memory_space=pltpu.VMEM)
SMEM = pl.BlockSpec(memory_space=pltpu.SMEM)
ANY = pl.BlockSpec(memory_space=pl.ANY)
DMA = pltpu.SemaphoreType.DMA


def solution(mesh):
    n_tp = mesh.shape['tp']
    n_chunks = 2

    def local_step(hidden, w_q, w_k, w_v, w_o, q_norm_w, k_norm_w, post_norm_w, k_cache, v_cache, positions):
        n_rows, width = hidden.shape
        slots, heads, head_dim = k_cache.shape[1:]
        cols = heads * head_dim
        depth = width // K_CHUNKS
        half = head_dim // 2
        inv_freq = ROPE_BASE ** (-2.0 * jnp.arange(half, dtype=F32) / head_dim)
        freq = jnp.concatenate([inv_freq, inv_freq])[None, :]
        sign = jnp.concatenate([-jnp.ones((half,), F32), jnp.ones((half,), F32)])[None, :]
        pos = positions.reshape(n_rows // LANES, LANES)
        by_head = jax.ShapeDtypeStruct((heads, n_rows, head_dim), BF16)
        q, k, v = pl.pallas_call(
            functools.partial(project_kernel, n_tp),
            out_shape=(by_head, by_head, by_head),
            in_specs=[ANY] * 4 + [VMEM] * 5,
            out_specs=(VMEM,) * 3,
            scratch_shapes=[
                pltpu.VMEM((K_CHUNKS, n_rows, depth), BF16),
                pltpu.VMEM((3 * K_CHUNKS, depth, cols), BF16),
                pltpu.VMEM((3, n_rows, cols), F32),
                pltpu.VMEM((n_rows, LANES), F32),
                pltpu.VMEM((n_rows, LANES), F32),
                pltpu.VMEM((8, n_rows), F32),
                pltpu.VMEM((n_tp - 1, 8, n_rows), F32),
                DMA((K_CHUNKS,)),
                DMA((3 * K_CHUNKS,)),
                DMA((n_tp - 1,)),
                DMA((n_tp - 1,)),
            ],
            compiler_params=pltpu.CompilerParams(collective_id=0, has_side_effects=True, vmem_limit_bytes=60 * 2**20),
            name='project',
        )(hidden, w_q, w_k, w_v, q_norm_w[None, :], k_norm_w[None, :], pos, freq, sign)

        flat = (n_rows * slots * heads, head_dim)
        n_groups = n_rows // GROUP
        k_new, v_new, o = pl.pallas_call(
            functools.partial(attend_kernel, slots, heads),
            out_shape=(jax.ShapeDtypeStruct(flat, BF16), jax.ShapeDtypeStruct(flat, BF16), jax.ShapeDtypeStruct((n_rows, cols), BF16)),
            in_specs=[SMEM] + [VMEM] * 4 + [ANY] * 2,
            out_specs=(ANY, ANY, VMEM),
            scratch_shapes=[
                pltpu.VMEM(flat, BF16),
                pltpu.VMEM(flat, BF16),
                pltpu.VMEM((n_rows * 8, head_dim), F32),
                pltpu.VMEM((n_rows * 8, head_dim), F32),
                pltpu.VMEM((n_rows, LANES), F32),
                DMA((2, n_groups)),
                DMA((2, n_groups)),
            ],
            compiler_params=pltpu.CompilerParams(vmem_limit_bytes=60 * 2**20),
            name='attend',
        )(positions, pos, q, k, v, k_cache.reshape(flat), v_cache.reshape(flat))

        blk = n_rows // n_chunks // n_tp
        side_rows = blk * (n_tp // 2)
        wide = width // 2
        out = pl.pallas_call(
            functools.partial(combine_kernel, n_tp, n_chunks),
            out_shape=jax.ShapeDtypeStruct((n_rows, width), BF16),
            in_specs=[VMEM, ANY, ANY, VMEM],
            out_specs=VMEM,
            scratch_shapes=[
                pltpu.VMEM((width // 512, cols, 512), BF16),
                pltpu.VMEM((2 * side_rows, cols), BF16),
                pltpu.VMEM((n_chunks, 2, side_rows, wide), BF16),
                pltpu.VMEM((n_chunks, 2, side_rows, wide), BF16),
                pltpu.VMEM((n_chunks, 2, side_rows, wide), F32),
                pltpu.VMEM((n_chunks, 2, blk, wide), BF16),
                pltpu.VMEM((n_chunks, 2, blk, wide), BF16),
                pltpu.VMEM((n_chunks, 2, 2, blk, wide), BF16),
                pltpu.VMEM((n_chunks, 2, 2, blk, wide), BF16),
                DMA((width // 512,)),
                DMA((n_chunks,)),
                pltpu.VMEM((n_chunks, blk, width), BF16),
            ] + [DMA((n_chunks, 2))] * 8 + [DMA((n_chunks, 9))] * 2,
            compiler_params=pltpu.CompilerParams(collective_id=1, has_side_effects=True, vmem_limit_bytes=60 * 2**20),
            name='combine',
        )(o, w_o, hidden, post_norm_w[None, :])
        return out, k_new.reshape(k_cache.shape), v_new.reshape(v_cache.shape)

    cache_spec = P('dp', None, 'tp', None)
    return jax.shard_map(local_step, mesh=mesh, in_specs=(P('dp', None), P(None, 'tp'), P(None, 'tp'), P(None, 'tp'), P('tp', None), P('tp'), P('tp'), P(None), cache_spec, cache_spec, P('dp')), out_specs=(P('dp', None), cache_spec, cache_spec), check_vma=False)
```
